32 devices in a mesh: gx: 8 (over y, x, core), gz: 4 (over z).
Axes of the slice: x: 2, y: 2, z: 4, core: 2. Of those that a mesh axis runs over, the one named last changes fastest.
Arguments:
- velocity: float32 [3, 64, 64, 512], P(None, 'gx', None, 'gz'), may hold values from -40 to 40
Outputs:
- coefficient: float32 [64], replicated
- eddy_viscosity: float32 [64, 64, 512], P('gx', None, 'gz')
The draws below stay inside these ranges and needn't reach their ends.
All inputs are finite; a program needn't handle non-finite values.
Results may differ from the reference program's by a relative error of at most 0.0001.
Values sent between devices are 32-bit elements; how exact they have to be, the bound alone decides.
A program may use at most 64 MiB of HBM per device.

```python
import jax
import jax.numpy as jnp
from jax import lax

NY = 64
NX = 64
NZ = 512


def draw_velocity(key, part):
    key_list = jax.random.split(key, 1)
    x_frac = jnp.arange(NX, dtype=jnp.float32) / NX
    z_frac = jnp.arange(NZ, dtype=jnp.float32) / NZ
    rising = jnp.exp(jnp.log(1.5) * (x_frac[:, None, None] + z_frac[None, None, :]))
    field = jax.random.truncated_normal(key_list[0], -6.0, 6.0, (3, NX, NY, NZ), jnp.float32) * rising
    return field.astype(jnp.float32)


def setup_inputs(seed: int = 0) -> dict:
    keys = jax.random.split(jax.random.key(seed), 2)
    velocity = draw_velocity(jax.random.fold_in(keys[1], 71), 0)
    return dict(velocity=velocity)


index_pairs = ((0, 0), (1, 1), (2, 2), (0, 1), (0, 2), (1, 2))
pair_weights = (1.0, 1.0, 1.0, 2.0, 2.0, 2.0)

def trim_edges(field):
    return field[..., 1:-1, :, 1:-1]

def along_x(field):
    return 0.5 * (field[..., 2:, :, 1:-1] - field[..., :-2, :, 1:-1])

def along_z(field):
    return 0.5 * (field[..., 1:-1, :, 2:] - field[..., 1:-1, :, :-2])

def along_y(field):
    inside = trim_edges(field)
    middle = 0.5 * (inside[..., 2:, :] - inside[..., :-2, :])
    bottom = inside[..., 1:2, :] - inside[..., 0:1, :]
    upper_end = inside[..., -1:, :] - inside[..., -2:-1, :]
    return jnp.concatenate([bottom, middle, upper_end], axis=-2)

def strain(velocity):
    gradients = [along_x(velocity), along_y(velocity), along_z(velocity)]
    strain_rate = jnp.stack([0.5 * (gradients[col_idx][row_idx] + gradients[row_idx][col_idx]) for row_idx, col_idx in index_pairs])
    weights = jnp.array(pair_weights, dtype=jnp.float32)[:, None, None, None]
    magnitude = jnp.sqrt(2.0 * lax.optimization_barrier(jnp.sum(weights * strain_rate * strain_rate, axis=0)))
    return (strain_rate, magnitude)

def box_filter(field):
    streamwise = 0.25 * (field[..., :-2, :, :] + 2.0 * field[..., 1:-1, :, :] + field[..., 2:, :, :])
    return 0.25 * (streamwise[..., :-2] + 2.0 * streamwise[..., 1:-1] + streamwise[..., 2:])

def wrap_pad(field):
    return jnp.pad(field, ((0, 0), (1, 1), (0, 0), (1, 1)), mode='wrap')

def reference(velocity):
    strain_rate, magnitude = strain(wrap_pad(velocity))
    filt_vel = box_filter(wrap_pad(velocity))
    test_rate, test_mag = strain(wrap_pad(filt_vel))
    numer = jnp.zeros((NY,), jnp.float32)
    denom = jnp.zeros((NY,), jnp.float32)
    for slot, (row_idx, col_idx) in enumerate(index_pairs):
        product = (velocity[row_idx] * velocity[col_idx])[None]
        filt_prod = box_filter(wrap_pad(product))[0]
        stress = (magnitude * strain_rate[slot])[None]
        filt_stress = box_filter(wrap_pad(stress))[0]
        leonard = filt_prod - filt_vel[row_idx] * filt_vel[col_idx]
        model_term = 2.0 * (filt_stress - 4.0 * test_mag * test_rate[slot])
        numer = numer + pair_weights[slot] * lax.optimization_barrier(jnp.sum(leonard * model_term, axis=(0, 2)))
        denom = denom + pair_weights[slot] * lax.optimization_barrier(jnp.sum(model_term * model_term, axis=(0, 2)))
    cells = NX * NZ
    coefficient = numer / cells / (denom / cells + 1e-06)
    eddy_viscosity = coefficient[None, :, None] * magnitude
    return (coefficient, eddy_viscosity)
```

```python
import functools

import jax
import jax.numpy as jnp
from jax import lax
from jax.experimental import pallas as pl
from jax.experimental.pallas import tpu as pltpu
from jax.sharding import PartitionSpec as P

pairs = ((0, 0), (1, 1), (2, 2), (0, 1), (0, 2), (1, 2))
PAD = 8
MESH = pl.DeviceIdType.MESH


def shear_terms(dx, dy, dz):
    terms = (dx[0], dy[1], dz[2], dx[1] + dy[0], dx[2] + dz[0], dy[2] + dz[1])
    square = [term * term for term in terms]
    total = 0.5 * (square[0] + square[1] + square[2]) + 0.25 * (square[3] + square[4] + square[5])
    return terms, jnp.sqrt(total)


def contraction(leonard, model):
    numer = leonard[0] * model[0]
    for slot in range(1, 6):
        numer = numer + leonard[slot] * model[slot]
    square = [term * term for term in model]
    denom = (square[0] + square[1] + square[2]) + 0.5 * (square[3] + square[4] + square[5])
    return numer, denom


def kernel(
    axes, sizes, cells, vel, coef_out, visc_out,
    U, HU, ST, MAG, ACC, G, RL, RR, row_mine, row_mid, got_x, got_z,
    load_sem, send_sem, recv_sem, sx_send, sx_recv, sz_send, sz_recv,
):
    nx, nz = sizes
    gx, gz = lax.axis_index(axes[0]), lax.axis_index(axes[1])
    X, Y, Z = vel.shape[1:]
    xl, xr = lax.rem(gx + nx - 1, nx), lax.rem(gx + 1, nx)
    zl, zr = lax.rem(gz + nz - 1, nz), lax.rem(gz + 1, nz)
    rows = pl.ds(PAD, Y)

    load = pltpu.make_async_copy(vel, U.at[:, pl.ds(2, X), rows, :], load_sem)
    load.start()

    barrier = pltpu.get_barrier_semaphore()
    peers = [(lax.rem(gx + k, nx), gz) for k in range(1, nx)]
    peers += [(gx, lax.rem(gz + k, nz)) for k in range(1, nz)]
    peers += [(a, b) for a in (xl, xr) for b in (zl, zr)]
    for peer in peers:
        pl.semaphore_signal(barrier, inc=1, device_id=peer, device_id_type=MESH)
    pl.semaphore_wait(barrier, len(peers))

    def send(slot, src, dst, peer):
        copy = pltpu.make_async_remote_copy(
            src_ref=src, dst_ref=dst, send_sem=send_sem.at[slot], recv_sem=recv_sem.at[slot],
            device_id=peer, device_id_type=MESH,
        )
        copy.start()
        return copy

    planes = [
        send(0, vel.at[:, pl.ds(0, 2)], U.at[:, pl.ds(X + 2, 2), rows, :], (xl, gz)),
        send(1, vel.at[:, pl.ds(X - 2, 2)], U.at[:, pl.ds(0, 2), rows, :], (xr, gz)),
    ]
    load.wait()

    lane = lax.broadcasted_iota(jnp.int32, (Y, Z), 1)
    for c in range(3):
        tile = jnp.zeros((Y, Z), jnp.float32)
        for x in range(X):
            rolled = pltpu.roll(U[c, x + 2, PAD:PAD + Y, :], (4 + 8 * x) % Z, 1)
            tile = jnp.where((lane >= 8 * x) & (lane < 8 * x + 8), rolled, tile)
        turned = jnp.concatenate([tile, tile], axis=0).T
        for x in range(X):
            G[c, x + 2] = turned[8 * x:8 * x + 8, :]

    mid, low, high = pl.ds(2, X), pl.ds(2, 2), pl.ds(X, 2)
    before, after = pl.ds(0, 2), pl.ds(X + 2, 2)
    edges = [
        send(2, G.at[:, low], G.at[:, after], (xl, gz)),
        send(3, G.at[:, high], G.at[:, before], (xr, gz)),
        send(4, G.at[:, mid], RL.at[:, mid], (gx, zr)),
        send(5, G.at[:, mid], RR.at[:, mid], (gx, zl)),
        send(6, G.at[:, low], RL.at[:, after], (xl, zr)),
        send(7, G.at[:, high], RL.at[:, before], (xr, zr)),
        send(8, G.at[:, low], RR.at[:, after], (xl, zl)),
        send(9, G.at[:, high], RR.at[:, before], (xr, zl)),
    ]

    def ghosts(ref, first, count):
        span = pl.ds(first, count)
        ref[:, span, PAD - 1:PAD, :] = (
            2.0 * ref[:, span, PAD:PAD + 1, :] - ref[:, span, PAD + 1:PAD + 2, :]
        )
        end = PAD + Y
        ref[:, span, end:end + 1, :] = (
            2.0 * ref[:, span, end - 1:end, :] - ref[:, span, end - 2:end - 1, :]
        )

    def z_sum(f):
        pair = f + pltpu.roll(f, 1, 1)
        return pair + pltpu.roll(pair, Z - 1, 1)

    def z_diff(f):
        return pltpu.roll(f, Z - 1, 1) - pltpu.roll(f, 1, 1)

    def stage_a(p):
        for r in range(PAD, PAD + Y, 8):
            u = [U[i, p, r:r + 8, :] for i in range(3)]
            up = [U[i, p + 1, r:r + 8, :] for i in range(3)]
            um = [U[i, p - 1, r:r + 8, :] for i in range(3)]
            dx = [up[i] - um[i] for i in range(3)]
            dy = [U[i, p, r + 1:r + 9, :] - U[i, p, r - 1:r + 7, :] for i in range(3)]
            dz = [z_diff(u[i]) for i in range(3)]
            terms, mag = shear_terms(dx, dy, dz)
            MAG[p, r - PAD:r - PAD + 8, :] = mag
            for slot in range(6):
                ST[slot, p, r - PAD:r - PAD + 8, :] = mag * terms[slot]
            for i in range(3):
                HU[i, p, r:r + 8, :] = 0.25 * z_sum((up[i] + um[i]) + 2.0 * u[i])
        ghosts(HU, p, 1)

    inner = lax.broadcasted_iota(jnp.int32, (8, Z), 1)
    inner = (inner >= 2) & (inner < Z - 2)

    def stage_b(p):
        for r in range(PAD, PAD + Y, 8):
            q = slice(r - PAD, r - PAD + 8)
            h = [HU[i, p, r:r + 8, :] for i in range(3)]
            dx = [HU[i, p + 1, r:r + 8, :] - HU[i, p - 1, r:r + 8, :] for i in range(3)]
            dy = [HU[i, p, r + 1:r + 9, :] - HU[i, p, r - 1:r + 7, :] for i in range(3)]
            dz = [z_diff(h[i]) for i in range(3)]
            terms, mag = shear_terms(dx, dy, dz)
            mag = 4.0 * mag
            u = [[U[i, p + k, r:r + 8, :] for i in range(3)] for k in (-1, 0, 1)]
            leonard, model = [], []
            for slot, (i, j) in enumerate(pairs):
                prod = (u[0][i] * u[0][j] + u[2][i] * u[2][j]) + 2.0 * (u[1][i] * u[1][j])
                leonard.append(z_sum(prod) - h[i] * h[j])
                stress = (ST[slot, p - 1, q, :] + ST[slot, p + 1, q, :]) + 2.0 * ST[slot, p, q, :]
                model.append(z_sum(stress) - mag * terms[slot])
            numer, denom = contraction(leonard, model)
            ACC[q, :] += jnp.where(inner, numer, 0.0)
            ACC[r - PAD + Y:r - PAD + Y + 8, :] += jnp.where(inner, denom, 0.0)

    def each(first, last, body):
        def step(p, carry):
            body(p)
            return carry

        lax.fori_loop(first, last, step, 0)

    ACC[...] = jnp.zeros_like(ACC)
    ghosts(U, 2, X)
    each(3, X + 1, stage_a)
    each(4, X, stage_b)
    for copy in planes:
        copy.wait_recv()
    ghosts(U, 0, 2)
    ghosts(U, X + 2, 2)
    each(0, 4, lambda s: stage_a(jnp.where(s < 2, s + 1, s + X - 1)))
    each(0, 4, lambda s: stage_b(jnp.where(s < 2, s + 2, s + X - 2)))

    for copy in edges:
        copy.wait_recv()
    W = X + 4
    ln = lax.broadcasted_iota(jnp.int32, (W, 8, 2 * Y), 2)
    sub = lax.broadcasted_iota(jnp.int32, (W, 8, 2 * Y), 1)
    left = ln < Y
    mine = left == (sub >= 4)

    def y_diff(f, n):
        y = ln[:n] - jnp.where(left[:n], 0, Y)
        plus, minus = pltpu.roll(f, 2 * Y - 1, 2), pltpu.roll(f, 1, 2)
        return jnp.where(y == Y - 1, 2.0 * f, jnp.where(y == 0, 2.0 * plus, plus)) - jnp.where(
            y == 0, 2.0 * f, jnp.where(y == Y - 1, 2.0 * minus, minus)
        )

    def s_diff(f):
        return pltpu.roll(f, 7, 1) - pltpu.roll(f, 1, 1)

    def s_sum(f):
        pair = f + pltpu.roll(f, 1, 1)
        return pair + pltpu.roll(pair, 7, 1)

    def x_sum(f):
        return (f[:-2] + f[2:]) + 2.0 * f[1:-1]

    w = [jnp.where(mine, G[c], jnp.where(left, RL[c], RR[c])) for c in range(3)]
    terms, wmag = shear_terms(
        [f[2:] - f[:-2] for f in w],
        [y_diff(f[1:-1], W - 2) for f in w],
        [s_diff(f[1:-1]) for f in w],
    )
    hw = [0.25 * s_sum(x_sum(f)) for f in w]
    test, tmag = shear_terms(
        [f[2:] - f[:-2] for f in hw],
        [y_diff(f[1:-1], X) for f in hw],
        [s_diff(f[1:-1]) for f in hw],
    )
    tmag = 4.0 * tmag
    leonard, model = [], []
    for slot, (i, j) in enumerate(pairs):
        prod = w[i][1:-1] * w[j][1:-1]
        leonard.append(s_sum(x_sum(prod)) - hw[i][1:-1] * hw[j][1:-1])
        model.append(s_sum(x_sum(wmag * terms[slot])) - tmag * test[slot])
    numer, denom = contraction(leonard, model)
    numer, denom = jnp.sum(numer, axis=0), jnp.sum(denom, axis=0)
    s2, l2 = sub[0], left[0]
    take = (l2 & ((s2 == 4) | (s2 == 5))) | (~l2 & ((s2 == 2) | (s2 == 3)))
    numer = jnp.sum(jnp.where(take, numer, 0.0), axis=0, keepdims=True)
    denom = jnp.sum(jnp.where(take, denom, 0.0), axis=0, keepdims=True)
    numer = numer + pltpu.roll(numer, Y, 1)
    denom = denom + pltpu.roll(denom, Y, 1)
    row_mine[...] = jnp.where(l2[:1], numer, denom) + jnp.sum(ACC[...].T, axis=0, keepdims=True)

    def share(mine_ref, got, axis_pos, me, count, ssem, rsem):
        copies = []
        for k in range(1, count):
            other = lax.rem(me + k, count)
            copy = pltpu.make_async_remote_copy(
                src_ref=mine_ref, dst_ref=got.at[k], send_sem=ssem.at[k], recv_sem=rsem.at[k],
                device_id=(other, gz) if axis_pos == 0 else (gx, other), device_id_type=MESH,
            )
            copy.start()
            copies.append(copy)
        return copies

    def gathered(mine_ref, got, copies):
        total = mine_ref[...]
        for k, copy in enumerate(copies):
            copy.wait_recv()
            total = total + got[k + 1]
        return total

    first = share(row_mine, got_x, 0, gx, nx, sx_send, sx_recv)

    back = wmag[1:-1].reshape(8 * X, 2 * Y)
    back = jnp.concatenate([back, jnp.zeros((Z - 8 * X, 2 * Y), jnp.float32)], axis=0).T
    for x in range(X):
        low_lane = pltpu.roll(back[:Y], (Z - 8 * x - 4) % Z, 1)
        high_lane = pltpu.roll(back[Y:], (Z - 1 - 8 * x - 3) % Z, 1)
        mag = MAG[x + 2]
        MAG[x + 2] = jnp.where(lane == 0, low_lane, jnp.where(lane == Z - 1, high_lane, mag))

    row_mid[...] = gathered(row_mine, got_x, first)
    second = share(row_mid, got_z, 1, gz, nz, sz_send, sz_recv)
    total = gathered(row_mid, got_z, second) * (1.0 / (256.0 * cells))
    coef = total / (pltpu.roll(total, Y, 1) + 1e-6)
    coef_out[...] = coef
    wide = jnp.broadcast_to(coef, (Z, 2 * Y)).T[:Y]
    for x in range(X):
        visc_out[x] = wide * MAG[x + 2]
    for copy in planes + edges + first + second:
        copy.wait_send()


def on_device(axes, sizes, velocity):
    X, Y, Z = velocity.shape[1:]
    nx, nz = sizes
    f32 = jnp.float32
    tall = Y + 2 * PAD
    W = X + 4
    dma = pltpu.SemaphoreType.DMA
    cells = X * nx * Z * nz
    coef, visc = pl.pallas_call(
        functools.partial(kernel, axes, sizes, cells),
        out_shape=(
            jax.ShapeDtypeStruct((1, 2 * Y), f32),
            jax.ShapeDtypeStruct((X, Y, Z), f32),
        ),
        in_specs=[pl.BlockSpec(memory_space=pl.ANY)],
        out_specs=(
            pl.BlockSpec(memory_space=pltpu.VMEM),
            pl.BlockSpec(memory_space=pltpu.VMEM),
        ),
        scratch_shapes=[
            pltpu.VMEM((3, W, tall, Z), f32),
            pltpu.VMEM((3, W, tall, Z), f32),
            pltpu.VMEM((6, W, Y, Z), f32),
            pltpu.VMEM((W, Y, Z), f32),
            pltpu.VMEM((2 * Y, Z), f32),
            pltpu.VMEM((3, W, 8, 2 * Y), f32),
            pltpu.VMEM((3, W, 8, 2 * Y), f32),
            pltpu.VMEM((3, W, 8, 2 * Y), f32),
            pltpu.VMEM((1, 2 * Y), f32),
            pltpu.VMEM((1, 2 * Y), f32),
            pltpu.VMEM((nx, 1, 2 * Y), f32),
            pltpu.VMEM((nz, 1, 2 * Y), f32),
            dma,
            dma((10,)),
            dma((10,)),
            dma((nx,)),
            dma((nx,)),
            dma((nz,)),
            dma((nz,)),
        ],
        compiler_params=pltpu.CompilerParams(collective_id=0, has_side_effects=True),
    )(velocity)
    return coef[0, :Y], visc


def solution(mesh):
    axes = ("gx", "gz")
    sizes = tuple(mesh.shape[axis] for axis in axes)
    return jax.shard_map(
        functools.partial(on_device, axes, sizes),
        mesh=mesh,
        in_specs=(P(None, "gx", None, "gz"),),
        out_specs=(P(), P("gx", None, "gz")),
        check_vma=False,
    )
```

```python
import functools

import jax
import jax.numpy as jnp
from jax import lax
from jax.experimental import pallas as pl
from jax.experimental.pallas import tpu as pltpu
from jax.sharding import PartitionSpec as P

pairs = ((0, 0), (1, 1), (2, 2), (0, 1), (0, 2), (1, 2))
PAD = 8
MESH = pl.DeviceIdType.MESH
EARLY_A = True


def shear_terms(dx, dy, dz):
    terms = (dx[0], dy[1], dz[2], dx[1] + dy[0], dx[2] + dz[0], dy[2] + dz[1])
    square = [term * term for term in terms]
    total = 0.5 * (square[0] + square[1] + square[2]) + 0.25 * (square[3] + square[4] + square[5])
    return terms, jnp.sqrt(total)


def contraction(leonard, model):
    numer = leonard[0] * model[0]
    for slot in range(1, 6):
        numer = numer + leonard[slot] * model[slot]
    square = [term * term for term in model]
    denom = (square[0] + square[1] + square[2]) + 0.5 * (square[3] + square[4] + square[5])
    return numer, denom


def kernel(
    axes, sizes, vel, sums_out, mag_out,
    U, HU, ST, MAG, ACC, LO, HI, RLO, RHI, BACK, GOT,
    load_sem, send_sem, recv_sem, sum_send, sum_recv,
):
    nx, nz = sizes
    count = nx * nz
    gx, gz = lax.axis_index(axes[0]), lax.axis_index(axes[1])
    X, Y, Z = vel.shape[1:]
    xl, xr = lax.rem(gx + nx - 1, nx), lax.rem(gx + 1, nx)
    zl, zr = lax.rem(gz + nz - 1, nz), lax.rem(gz + 1, nz)
    rows = pl.ds(PAD, Y)
    me = gx * nz + gz

    load = pltpu.make_async_copy(vel, U.at[:, pl.ds(2, X), rows, :], load_sem)
    load.start()

    def to_all(body):
        def step(k, carry):
            body((lax.rem(gx + k // nz, nx), lax.rem(gz + lax.rem(k, nz), nz)))
            return carry

        lax.fori_loop(1, count, step, 0, unroll=min(count - 1, 31))

    barrier = pltpu.get_barrier_semaphore()
    to_all(lambda peer: pl.semaphore_signal(barrier, inc=1, device_id=peer, device_id_type=MESH))

    def send(slot, src, dst, peer):
        copy = pltpu.make_async_remote_copy(
            src_ref=src, dst_ref=dst, send_sem=send_sem.at[slot], recv_sem=recv_sem.at[slot],
            device_id=peer, device_id_type=MESH,
        )
        copy.start()
        return copy

    load.wait()

    lane = lax.broadcasted_iota(jnp.int32, (Y, Z), 1)
    span = 4 * X
    for c in range(3):
        tile = jnp.zeros((Y, Z), jnp.float32)
        for x in range(X):
            plane = U[c, x + 2, PAD:PAD + Y, :]
            top = pltpu.roll(plane, (4 + 4 * x) % Z, 1)
            bottom = pltpu.roll(plane, span + 4 * x, 1)
            tile = jnp.where((lane >= 4 * x) & (lane < 4 * x + 4), top, tile)
            tile = jnp.where((lane >= span + 4 * x) & (lane < span + 4 * x + 4), bottom, tile)
        turned = jnp.concatenate([tile, tile], axis=0).T
        for t in range(X // 2):
            LO[c, t + 1] = turned[8 * t:8 * t + 8, :]
            HI[c, t + 1] = turned[span + 8 * t:span + 8 * t + 8, :]

    def ghosts(ref, first, count):
        span = pl.ds(first, count)
        ref[:, span, PAD - 1:PAD, :] = (
            2.0 * ref[:, span, PAD:PAD + 1, :] - ref[:, span, PAD + 1:PAD + 2, :]
        )
        end = PAD + Y
        ref[:, span, end:end + 1, :] = (
            2.0 * ref[:, span, end - 1:end, :] - ref[:, span, end - 2:end - 1, :]
        )

    def z_sum(f):
        pair = f + pltpu.roll(f, 1, 1)
        return pair + pltpu.roll(pair, Z - 1, 1)

    def z_diff(f):
        return pltpu.roll(f, Z - 1, 1) - pltpu.roll(f, 1, 1)

    def stage_a(p):
        for r in range(PAD, PAD + Y, 8):
            u = [U[i, p, r:r + 8, :] for i in range(3)]
            up = [U[i, p + 1, r:r + 8, :] for i in range(3)]
            um = [U[i, p - 1, r:r + 8, :] for i in range(3)]
            dx = [up[i] - um[i] for i in range(3)]
            dy = [U[i, p, r + 1:r + 9, :] - U[i, p, r - 1:r + 7, :] for i in range(3)]
            dz = [z_diff(u[i]) for i in range(3)]
            terms, mag = shear_terms(dx, dy, dz)
            MAG[p, r - PAD:r - PAD + 8, :] = mag
            for slot in range(6):
                ST[slot, p, r - PAD:r - PAD + 8, :] = mag * terms[slot]
            for i in range(3):
                HU[i, p, r:r + 8, :] = 0.25 * z_sum((up[i] + um[i]) + 2.0 * u[i])
        ghosts(HU, p, 1)

    inner = lax.broadcasted_iota(jnp.int32, (8, Z), 1)
    inner = (inner >= 2) & (inner < Z - 2)

    def stage_b(p):
        for r in range(PAD, PAD + Y, 8):
            q = slice(r - PAD, r - PAD + 8)
            h = [HU[i, p, r:r + 8, :] for i in range(3)]
            dx = [HU[i, p + 1, r:r + 8, :] - HU[i, p - 1, r:r + 8, :] for i in range(3)]
            dy = [HU[i, p, r + 1:r + 9, :] - HU[i, p, r - 1:r + 7, :] for i in range(3)]
            dz = [z_diff(h[i]) for i in range(3)]
            terms, mag = shear_terms(dx, dy, dz)
            mag = 4.0 * mag
            u = [[U[i, p + k, r:r + 8, :] for i in range(3)] for k in (-1, 0, 1)]
            leonard, model = [], []
            for slot, (i, j) in enumerate(pairs):
                prod = (u[0][i] * u[0][j] + u[2][i] * u[2][j]) + 2.0 * (u[1][i] * u[1][j])
                leonard.append(z_sum(prod) - h[i] * h[j])
                stress = (ST[slot, p - 1, q, :] + ST[slot, p + 1, q, :]) + 2.0 * ST[slot, p, q, :]
                model.append(z_sum(stress) - mag * terms[slot])
            numer, denom = contraction(leonard, model)
            ACC[q, :] += jnp.where(inner, numer, 0.0)
            ACC[r - PAD + Y:r - PAD + Y + 8, :] += jnp.where(inner, denom, 0.0)

    def each(first, last, body):
        def step(p, carry):
            body(p)
            return carry

        lax.fori_loop(first, last, step, 0)

    ACC[...] = jnp.zeros_like(ACC)
    ghosts(U, 2, X)
    if EARLY_A:
        each(3, X + 1, stage_a)
    pl.semaphore_wait(barrier, count - 1)

    half = X // 2
    mid, low, high = pl.ds(1, half), pl.ds(1, 1), pl.ds(half, 1)
    before, after = pl.ds(0, 1), pl.ds(half + 1, 1)
    edges = [
        send(0, LO.at[:, low], RLO.at[:, after], (xl, zr)),
        send(1, LO.at[:, high], RLO.at[:, before], (xr, zr)),
        send(2, HI.at[:, low], RHI.at[:, after], (xl, zl)),
        send(3, HI.at[:, high], RHI.at[:, before], (xr, zl)),
        send(4, LO.at[:, mid], RLO.at[:, mid], (gx, zr)),
        send(5, HI.at[:, mid], RHI.at[:, mid], (gx, zl)),
        send(6, LO.at[:, low], LO.at[:, after], (xl, gz)),
        send(7, LO.at[:, high], LO.at[:, before], (xr, gz)),
        send(8, HI.at[:, low], HI.at[:, after], (xl, gz)),
        send(9, HI.at[:, high], HI.at[:, before], (xr, gz)),
    ]

    def send_plane(slot, x, ext, peer):
        return send(slot, vel.at[:, pl.ds(x, 1)], U.at[:, pl.ds(ext, 1), rows, :], peer)

    near = [send_plane(10, 0, X + 2, (xl, gz)), send_plane(11, X - 1, 1, (xr, gz))]
    far = [send_plane(12, 1, X + 3, (xl, gz)), send_plane(13, X - 2, 0, (xr, gz))]

    if not EARLY_A:
        each(3, X + 1, stage_a)
    each(4, X, stage_b)

    for copy in edges:
        copy.wait_recv()
    W = X + 4
    ln = lax.broadcasted_iota(jnp.int32, (W, 8, 2 * Y), 2)
    sub = lax.broadcasted_iota(jnp.int32, (W, 8, 2 * Y), 1)
    left = ln < Y

    def y_diff(f, n):
        y = ln[:n] - jnp.where(left[:n], 0, Y)
        plus, minus = pltpu.roll(f, 2 * Y - 1, 2), pltpu.roll(f, 1, 2)
        return jnp.where(y == Y - 1, 2.0 * f, jnp.where(y == 0, 2.0 * plus, plus)) - jnp.where(
            y == 0, 2.0 * f, jnp.where(y == Y - 1, 2.0 * minus, minus)
        )

    def s_diff(f):
        return pltpu.roll(f, 7, 1) - pltpu.roll(f, 1, 1)

    def s_sum(f):
        pair = f + pltpu.roll(f, 1, 1)
        return pair + pltpu.roll(pair, 7, 1)

    def x_sum(f):
        return (f[:-2] + f[2:]) + 2.0 * f[1:-1]

    w = []
    head = sub[:2] < 4
    for c in range(3):
        found = []
        for t in range(W // 2):
            upper = jnp.where(left[0], RLO[c, t], LO[c, t])
            lower = jnp.where(left[0], HI[c, t], RHI[c, t])
            found.append(jnp.where(head[0], upper, pltpu.roll(lower, 4, 0)))
            found.append(jnp.where(head[0], pltpu.roll(upper, 4, 0), lower))
        w.append(jnp.stack(found))
    terms, wmag = shear_terms(
        [f[2:] - f[:-2] for f in w],
        [y_diff(f[1:-1], W - 2) for f in w],
        [s_diff(f[1:-1]) for f in w],
    )
    hw = [0.25 * s_sum(x_sum(f)) for f in w]
    test, tmag = shear_terms(
        [f[2:] - f[:-2] for f in hw],
        [y_diff(f[1:-1], X) for f in hw],
        [s_diff(f[1:-1]) for f in hw],
    )
    tmag = 4.0 * tmag
    leonard, model = [], []
    for slot, (i, j) in enumerate(pairs):
        prod = w[i][1:-1] * w[j][1:-1]
        leonard.append(s_sum(x_sum(prod)) - hw[i][1:-1] * hw[j][1:-1])
        model.append(s_sum(x_sum(wmag * terms[slot])) - tmag * test[slot])
    numer, denom = contraction(leonard, model)
    numer, denom = jnp.sum(numer, axis=0), jnp.sum(denom, axis=0)
    s2, l2 = sub[0], left[0]
    take = (l2 & ((s2 == 4) | (s2 == 5))) | (~l2 & ((s2 == 2) | (s2 == 3)))
    numer = jnp.sum(jnp.where(take, numer, 0.0), axis=0, keepdims=True)
    denom = jnp.sum(jnp.where(take, denom, 0.0), axis=0, keepdims=True)
    numer = numer + pltpu.roll(numer, Y, 1)
    denom = denom + pltpu.roll(denom, Y, 1)
    window_sums = jnp.where(l2[:1], numer, denom)

    back = wmag[1:-1].reshape(8 * X, 2 * Y)
    back = jnp.concatenate([back, jnp.zeros((Z - 8 * X, 2 * Y), jnp.float32)], axis=0).T
    BACK[...] = back

    for copy in near:
        copy.wait_recv()
    ghosts(U, 1, 1)
    ghosts(U, X + 2, 1)
    each(0, 2, lambda s: stage_a(2 + s * (X - 1)))
    each(0, 2, lambda s: stage_b(3 + s * (X - 3)))
    for copy in far:
        copy.wait_recv()
    ghosts(U, 0, 1)
    ghosts(U, X + 3, 1)
    each(0, 2, lambda s: stage_a(1 + s * (X + 1)))
    each(0, 2, lambda s: stage_b(2 + s * (X - 1)))

    GOT[me] = window_sums + jnp.sum(ACC[...].T, axis=0, keepdims=True)

    def total_copy(peer):
        return pltpu.make_async_remote_copy(
            src_ref=GOT.at[me], dst_ref=GOT.at[me], send_sem=sum_send, recv_sem=sum_recv,
            device_id=peer, device_id_type=MESH,
        )

    to_all(lambda peer: total_copy(peer).start())
    for x in range(X):
        low_lane = pltpu.roll(BACK[:Y], (Z - 8 * x - 4) % Z, 1)
        high_lane = pltpu.roll(BACK[Y:], (Z - 1 - 8 * x - 3) % Z, 1)
        mag = MAG[x + 2]
        mag_out[x] = jnp.where(lane == 0, low_lane, jnp.where(lane == Z - 1, high_lane, mag))
    for copy in edges + near + far:
        copy.wait_send()
    everyone = GOT.at[pl.ds(0, count - 1)]
    pltpu.make_async_copy(everyone, everyone, sum_recv).wait()
    sums_out[...] = jnp.sum(GOT[...], axis=0)
    pltpu.make_async_copy(everyone, everyone, sum_send).wait()


def finish(cells, sums, mag, coef_out, visc_out):
    X, Y, Z = mag.shape
    total = sums[...] * (1.0 / (256.0 * cells))
    coef = total / (pltpu.roll(total, Y, 1) + 1e-6)
    coef_out[...] = coef[0, :Y]
    wide = jnp.broadcast_to(coef, (Z, 2 * Y)).T[:Y]
    for x in range(X):
        visc_out[x] = wide * mag[x]


def on_device(axes, sizes, velocity):
    X, Y, Z = velocity.shape[1:]
    nx, nz = sizes
    f32 = jnp.float32
    tall = Y + 2 * PAD
    W = X + 4
    dma = pltpu.SemaphoreType.DMA
    cells = X * nx * Z * nz
    vmem = pl.BlockSpec(memory_space=pltpu.VMEM)
    strip = pltpu.VMEM((3, W // 2, 8, 2 * Y), f32)
    sums, mag = pl.pallas_call(
        functools.partial(kernel, axes, sizes),
        out_shape=(
            jax.ShapeDtypeStruct((1, 2 * Y), f32),
            jax.ShapeDtypeStruct((X, Y, Z), f32),
        ),
        in_specs=[pl.BlockSpec(memory_space=pl.ANY)],
        out_specs=(vmem, vmem),
        scratch_shapes=[
            pltpu.VMEM((3, W, tall, Z), f32),
            pltpu.VMEM((3, W, tall, Z), f32),
            pltpu.VMEM((6, W, Y, Z), f32),
            pltpu.VMEM((W, Y, Z), f32),
            pltpu.VMEM((2 * Y, Z), f32),
            strip,
            strip,
            strip,
            strip,
            pltpu.VMEM((2 * Y, Z), f32),
            pltpu.VMEM((nx * nz, 1, 2 * Y), f32),
            dma,
            dma((14,)),
            dma((14,)),
            dma,
            dma,
        ],
        compiler_params=pltpu.CompilerParams(collective_id=0, has_side_effects=True),
    )(velocity)
    return pl.pallas_call(
        functools.partial(finish, cells),
        out_shape=(jax.ShapeDtypeStruct((Y,), f32), jax.ShapeDtypeStruct((X, Y, Z), f32)),
        in_specs=[vmem, vmem],
        out_specs=(vmem, vmem),
    )(sums, mag)


def solution(mesh):
    axes = ("gx", "gz")
    sizes = tuple(mesh.shape[axis] for axis in axes)
    return jax.shard_map(
        functools.partial(on_device, axes, sizes),
        mesh=mesh,
        in_specs=(P(None, "gx", None, "gz"),),
        out_specs=(P(), P("gx", None, "gz")),
        check_vma=False,
    )
```

```python
import functools

import jax
import jax.numpy as jnp
from jax import lax
from jax.experimental import pallas as pl
from jax.experimental.pallas import tpu as pltpu
from jax.sharding import PartitionSpec as P

pairs = ((0, 0), (1, 1), (2, 2), (0, 1), (0, 2), (1, 2))
PAD = 8
MESH = pl.DeviceIdType.MESH
EARLY_A = False


def shear_terms(dx, dy, dz):
    terms = (dx[0], dy[1], dz[2], dx[1] + dy[0], dx[2] + dz[0], dy[2] + dz[1])
    square = [term * term for term in terms]
    total = 0.5 * (square[0] + square[1] + square[2]) + 0.25 * (square[3] + square[4] + square[5])
    return terms, jnp.sqrt(total)


def contraction(leonard, model):
    numer = leonard[0] * model[0]
    for slot in range(1, 6):
        numer = numer + leonard[slot] * model[slot]
    square = [term * term for term in model]
    denom = (square[0] + square[1] + square[2]) + 0.5 * (square[3] + square[4] + square[5])
    return numer, denom


def kernel(
    axes, sizes, vel, sums_out, mag_out,
    U, HU, ST, MAG, ACC, LO, HI, RLO, RHI, BACK, GOT,
    load_sem, send_sem, recv_sem, sum_send, sum_recv,
):
    nx, nz = sizes
    count = nx * nz
    gx, gz = lax.axis_index(axes[0]), lax.axis_index(axes[1])
    X, Y, Z = vel.shape[1:]
    xl, xr = lax.rem(gx + nx - 1, nx), lax.rem(gx + 1, nx)
    zl, zr = lax.rem(gz + nz - 1, nz), lax.rem(gz + 1, nz)
    rows = pl.ds(PAD, Y)
    me = gx * nz + gz

    load = pltpu.make_async_copy(vel, U.at[:, pl.ds(2, X), rows, :], load_sem)
    load.start()

    def to_all(body):
        def step(k, carry):
            body((lax.rem(gx + k // nz, nx), lax.rem(gz + lax.rem(k, nz), nz)))
            return carry

        lax.fori_loop(1, count, step, 0, unroll=min(count - 1, 31))

    barrier = pltpu.get_barrier_semaphore()
    to_all(lambda peer: pl.semaphore_signal(barrier, inc=1, device_id=peer, device_id_type=MESH))

    def send(slot, src, dst, peer):
        copy = pltpu.make_async_remote_copy(
            src_ref=src, dst_ref=dst, send_sem=send_sem.at[slot], recv_sem=recv_sem.at[slot],
            device_id=peer, device_id_type=MESH,
        )
        copy.start()
        return copy

    load.wait()

    lane = lax.broadcasted_iota(jnp.int32, (Y, Z), 1)
    span = 4 * X
    for c in range(3):
        tile = jnp.zeros((Y, Z), jnp.float32)
        for x in range(X):
            plane = U[c, x + 2, PAD:PAD + Y, :]
            top = pltpu.roll(plane, (4 + 4 * x) % Z, 1)
            bottom = pltpu.roll(plane, span + 4 * x, 1)
            tile = jnp.where((lane >= 4 * x) & (lane < 4 * x + 4), top, tile)
            tile = jnp.where((lane >= span + 4 * x) & (lane < span + 4 * x + 4), bottom, tile)
        turned = jnp.concatenate([tile, tile], axis=0).T
        for t in range(X // 2):
            LO[c, t + 1] = turned[8 * t:8 * t + 8, :]
            HI[c, t + 1] = turned[span + 8 * t:span + 8 * t + 8, :]

    def ghosts(ref, first, count):
        span = pl.ds(first, count)
        ref[:, span, PAD - 1:PAD, :] = (
            2.0 * ref[:, span, PAD:PAD + 1, :] - ref[:, span, PAD + 1:PAD + 2, :]
        )
        end = PAD + Y
        ref[:, span, end:end + 1, :] = (
            2.0 * ref[:, span, end - 1:end, :] - ref[:, span, end - 2:end - 1, :]
        )

    def z_sum(f):
        pair = f + pltpu.roll(f, 1, 1)
        return pair + pltpu.roll(pair, Z - 1, 1)

    def z_diff(f):
        return pltpu.roll(f, Z - 1, 1) - pltpu.roll(f, 1, 1)

    def stage_a(p):
        for r in range(PAD, PAD + Y, 8):
            u = [U[i, p, r:r + 8, :] for i in range(3)]
            up = [U[i, p + 1, r:r + 8, :] for i in range(3)]
            um = [U[i, p - 1, r:r + 8, :] for i in range(3)]
            dx = [up[i] - um[i] for i in range(3)]
            dy = [U[i, p, r + 1:r + 9, :] - U[i, p, r - 1:r + 7, :] for i in range(3)]
            dz = [z_diff(u[i]) for i in range(3)]
            terms, mag = shear_terms(dx, dy, dz)
            MAG[p, r - PAD:r - PAD + 8, :] = mag
            for slot in range(6):
                ST[slot, p, r - PAD:r - PAD + 8, :] = mag * terms[slot]
            for i in range(3):
                HU[i, p, r:r + 8, :] = 0.25 * z_sum((up[i] + um[i]) + 2.0 * u[i])
        ghosts(HU, p, 1)

    inner = lax.broadcasted_iota(jnp.int32, (8, Z), 1)
    inner = (inner >= 2) & (inner < Z - 2)

    def stage_b(p):
        for r in range(PAD, PAD + Y, 8):
            q = slice(r - PAD, r - PAD + 8)
            h = [HU[i, p, r:r + 8, :] for i in range(3)]
            dx = [HU[i, p + 1, r:r + 8, :] - HU[i, p - 1, r:r + 8, :] for i in range(3)]
            dy = [HU[i, p, r + 1:r + 9, :] - HU[i, p, r - 1:r + 7, :] for i in range(3)]
            dz = [z_diff(h[i]) for i in range(3)]
            terms, mag = shear_terms(dx, dy, dz)
            mag = 4.0 * mag
            u = [[U[i, p + k, r:r + 8, :] for i in range(3)] for k in (-1, 0, 1)]
            leonard, model = [], []
            for slot, (i, j) in enumerate(pairs):
                prod = (u[0][i] * u[0][j] + u[2][i] * u[2][j]) + 2.0 * (u[1][i] * u[1][j])
                leonard.append(z_sum(prod) - h[i] * h[j])
                stress = (ST[slot, p - 1, q, :] + ST[slot, p + 1, q, :]) + 2.0 * ST[slot, p, q, :]
                model.append(z_sum(stress) - mag * terms[slot])
            numer, denom = contraction(leonard, model)
            ACC[q, :] += jnp.where(inner, numer, 0.0)
            ACC[r - PAD + Y:r - PAD + Y + 8, :] += jnp.where(inner, denom, 0.0)

    def each(first, last, body):
        def step(p, carry):
            body(p)
            return carry

        lax.fori_loop(first, last, step, 0)

    ACC[...] = jnp.zeros_like(ACC)
    ghosts(U, 2, X)
    if EARLY_A:
        each(3, X + 1, stage_a)
    pl.semaphore_wait(barrier, count - 1)

    half = X // 2
    mid, low, high = pl.ds(1, half), pl.ds(1, 1), pl.ds(half, 1)
    before, after = pl.ds(0, 1), pl.ds(half + 1, 1)
    edges = [
        send(0, LO.at[:, low], RLO.at[:, after], (xl, zr)),
        send(1, LO.at[:, high], RLO.at[:, before], (xr, zr)),
        send(2, HI.at[:, low], RHI.at[:, after], (xl, zl)),
        send(3, HI.at[:, high], RHI.at[:, before], (xr, zl)),
        send(4, LO.at[:, mid], RLO.at[:, mid], (gx, zr)),
        send(5, HI.at[:, mid], RHI.at[:, mid], (gx, zl)),
        send(6, LO.at[:, low], LO.at[:, after], (xl, gz)),
        send(7, LO.at[:, high], LO.at[:, before], (xr, gz)),
        send(8, HI.at[:, low], HI.at[:, after], (xl, gz)),
        send(9, HI.at[:, high], HI.at[:, before], (xr, gz)),
    ]

    def send_plane(slot, x, ext, peer):
        return send(slot, vel.at[:, pl.ds(x, 1)], U.at[:, pl.ds(ext, 1), rows, :], peer)

    near = [send_plane(10, 0, X + 2, (xl, gz)), send_plane(11, X - 1, 1, (xr, gz))]
    far = [send_plane(12, 1, X + 3, (xl, gz)), send_plane(13, X - 2, 0, (xr, gz))]

    if not EARLY_A:
        each(3, X + 1, stage_a)
    each(4, X, stage_b)

    for copy in near:
        copy.wait_recv()
    ghosts(U, 1, 1)
    ghosts(U, X + 2, 1)
    each(0, 2, lambda s: stage_a(2 + s * (X - 1)))
    each(0, 2, lambda s: stage_b(3 + s * (X - 3)))
    for copy in edges:
        copy.wait_recv()
    W = X + 4
    ln = lax.broadcasted_iota(jnp.int32, (W, 8, 2 * Y), 2)
    sub = lax.broadcasted_iota(jnp.int32, (W, 8, 2 * Y), 1)
    left = ln < Y

    def y_diff(f, n):
        y = ln[:n] - jnp.where(left[:n], 0, Y)
        plus, minus = pltpu.roll(f, 2 * Y - 1, 2), pltpu.roll(f, 1, 2)
        return jnp.where(y == Y - 1, 2.0 * f, jnp.where(y == 0, 2.0 * plus, plus)) - jnp.where(
            y == 0, 2.0 * f, jnp.where(y == Y - 1, 2.0 * minus, minus)
        )

    def s_diff(f):
        return pltpu.roll(f, 7, 1) - pltpu.roll(f, 1, 1)

    def s_sum(f):
        pair = f + pltpu.roll(f, 1, 1)
        return pair + pltpu.roll(pair, 7, 1)

    def x_sum(f):
        return (f[:-2] + f[2:]) + 2.0 * f[1:-1]

    w = []
    head = sub[:2] < 4
    for c in range(3):
        found = []
        for t in range(W // 2):
            upper = jnp.where(left[0], RLO[c, t], LO[c, t])
            lower = jnp.where(left[0], HI[c, t], RHI[c, t])
            found.append(jnp.where(head[0], upper, pltpu.roll(lower, 4, 0)))
            found.append(jnp.where(head[0], pltpu.roll(upper, 4, 0), lower))
        w.append(jnp.stack(found))
    terms, wmag = shear_terms(
        [f[2:] - f[:-2] for f in w],
        [y_diff(f[1:-1], W - 2) for f in w],
        [s_diff(f[1:-1]) for f in w],
    )
    hw = [0.25 * s_sum(x_sum(f)) for f in w]
    test, tmag = shear_terms(
        [f[2:] - f[:-2] for f in hw],
        [y_diff(f[1:-1], X) for f in hw],
        [s_diff(f[1:-1]) for f in hw],
    )
    tmag = 4.0 * tmag
    leonard, model = [], []
    for slot, (i, j) in enumerate(pairs):
        prod = w[i][1:-1] * w[j][1:-1]
        leonard.append(s_sum(x_sum(prod)) - hw[i][1:-1] * hw[j][1:-1])
        model.append(s_sum(x_sum(wmag * terms[slot])) - tmag * test[slot])
    numer, denom = contraction(leonard, model)
    numer, denom = jnp.sum(numer, axis=0), jnp.sum(denom, axis=0)
    s2, l2 = sub[0], left[0]
    take = (l2 & ((s2 == 4) | (s2 == 5))) | (~l2 & ((s2 == 2) | (s2 == 3)))
    numer = jnp.sum(jnp.where(take, numer, 0.0), axis=0, keepdims=True)
    denom = jnp.sum(jnp.where(take, denom, 0.0), axis=0, keepdims=True)
    numer = numer + pltpu.roll(numer, Y, 1)
    denom = denom + pltpu.roll(denom, Y, 1)
    window_sums = jnp.where(l2[:1], numer, denom)

    back = wmag[1:-1].reshape(8 * X, 2 * Y)
    back = jnp.concatenate([back, jnp.zeros((Z - 8 * X, 2 * Y), jnp.float32)], axis=0).T
    BACK[...] = back

    for copy in far:
        copy.wait_recv()
    ghosts(U, 0, 1)
    ghosts(U, X + 3, 1)
    each(0, 2, lambda s: stage_a(1 + s * (X + 1)))
    each(0, 2, lambda s: stage_b(2 + s * (X - 1)))

    GOT[me] = window_sums + jnp.sum(ACC[...].T, axis=0, keepdims=True)

    def total_copy(peer):
        return pltpu.make_async_remote_copy(
            src_ref=GOT.at[me], dst_ref=GOT.at[me], send_sem=sum_send, recv_sem=sum_recv,
            device_id=peer, device_id_type=MESH,
        )

    to_all(lambda peer: total_copy(peer).start())
    for x in range(X):
        low_lane = pltpu.roll(BACK[:Y], (Z - 8 * x - 4) % Z, 1)
        high_lane = pltpu.roll(BACK[Y:], (Z - 1 - 8 * x - 3) % Z, 1)
        mag = MAG[x + 2]
        mag_out[x] = jnp.where(lane == 0, low_lane, jnp.where(lane == Z - 1, high_lane, mag))
    for copy in edges + near + far:
        copy.wait_send()
    everyone = GOT.at[pl.ds(0, count - 1)]
    pltpu.make_async_copy(everyone, everyone, sum_recv).wait()
    sums_out[...] = jnp.sum(GOT[...], axis=0)
    pltpu.make_async_copy(everyone, everyone, sum_send).wait()


def finish(cells, sums, mag, coef_out, visc_out):
    X, Y, Z = mag.shape
    total = sums[...] * (1.0 / (256.0 * cells))
    coef = total / (pltpu.roll(total, Y, 1) + 1e-6)
    coef_out[...] = coef[0, :Y]
    wide = jnp.broadcast_to(coef, (Z, 2 * Y)).T[:Y]
    for x in range(X):
        visc_out[x] = wide * mag[x]


def on_device(axes, sizes, velocity):
    X, Y, Z = velocity.shape[1:]
    nx, nz = sizes
    f32 = jnp.float32
    tall = Y + 2 * PAD
    W = X + 4
    dma = pltpu.SemaphoreType.DMA
    cells = X * nx * Z * nz
    vmem = pl.BlockSpec(memory_space=pltpu.VMEM)
    strip = pltpu.VMEM((3, W // 2, 8, 2 * Y), f32)
    sums, mag = pl.pallas_call(
        functools.partial(kernel, axes, sizes),
        out_shape=(pltpu.VMEM((1, 2 * Y), f32), pltpu.VMEM((X, Y, Z), f32)),
        in_specs=[pl.BlockSpec(memory_space=pl.ANY)],
        out_specs=(vmem, vmem),
        scratch_shapes=[
            pltpu.VMEM((3, W, tall, Z), f32),
            pltpu.VMEM((3, W, tall, Z), f32),
            pltpu.VMEM((6, W, Y, Z), f32),
            pltpu.VMEM((W, Y, Z), f32),
            pltpu.VMEM((2 * Y, Z), f32),
            strip,
            strip,
            strip,
            strip,
            pltpu.VMEM((2 * Y, Z), f32),
            pltpu.VMEM((nx * nz, 1, 2 * Y), f32),
            dma,
            dma((14,)),
            dma((14,)),
            dma,
            dma,
        ],
        compiler_params=pltpu.CompilerParams(collective_id=0, has_side_effects=True),
    )(velocity)
    return pl.pallas_call(
        functools.partial(finish, cells),
        out_shape=(jax.ShapeDtypeStruct((Y,), f32), jax.ShapeDtypeStruct((X, Y, Z), f32)),
        in_specs=[vmem, vmem],
        out_specs=(vmem, vmem),
    )(*(pltpu.with_memory_space_constraint(a, pltpu.VMEM) for a in (sums, mag)))


def solution(mesh):
    axes = ("gx", "gz")
    sizes = tuple(mesh.shape[axis] for axis in axes)
    return jax.shard_map(
        functools.partial(on_device, axes, sizes),
        mesh=mesh,
        in_specs=(P(None, "gx", None, "gz"),),
        out_specs=(P(), P("gx", None, "gz")),
        check_vma=False,
    )
```
